128 devices in a mesh: expert: 4 (over y), shard: 32 (over z, x, core).
Axes of the slice: x: 4, y: 4, z: 4, core: 2. Of those that a mesh axis runs over, the one named last changes fastest.
Arguments:
- master_gate: float32 [64, 2048, 1408], P('expert', 'shard'), may hold values from -0.25 to 0.25
- master_up: float32 [64, 2048, 1408], P('expert', 'shard'), may hold values from -0.25 to 0.25
- master_down: float32 [64, 1408, 2048], P('expert', None, 'shard'), may hold values from -0.3125 to 0.3125
- router_weight: float32 [2048, 64], P('shard', 'expert'), may hold values from -0.125 to 0.125
- router_gain: float32 [2048], P('shard'), may hold values from 0.25 to 1.75
Outputs:
- final_gate: bfloat16 [64, 2048, 1408], P('expert', None, 'shard')
- final_up: bfloat16 [64, 2048, 1408], P('expert', None, 'shard')
- final_down: bfloat16 [64, 1408, 2048], P('expert', 'shard')
- scale_gate: float32 [64, 1408], P('expert', 'shard')
- scale_up: float32 [64, 1408], P('expert', 'shard')
- scale_down: float32 [64, 1408], P('expert', 'shard')
- serve_router: bfloat16 [2048, 64], replicated
The draws below stay inside these ranges and needn't reach their ends.
All inputs are finite; a program needn't handle non-finite values. Where the reference program divides by a largest or mean magnitude, that divisor is 1e-20 or more.
Results may differ from the reference program's by a relative error of at most 0.001.
Values may be sent and summed in bfloat16 or wider, within the bound.
A program may use at most 192 MiB of HBM per device.

```python
import jax
import jax.numpy as jnp

EXPERTS = 64
D_MODEL = 2048
D_EXPERT = 1408


def with_spikes(drawn, stream_key, source, target, shards_of, factor):
    owner, partner = [(jnp.arange(drawn.shape[position]) // (drawn.shape[position] // shards_of)).reshape([-1 if axis == position else 1 for axis in range(drawn.ndim)]) for position in (source, target)]
    chosen = jax.random.permutation(stream_key, shards_of)[partner]
    strong = (owner == chosen) | (owner == (partner + shards_of // 2) % shards_of)
    return jnp.where(strong, factor * drawn, drawn)


def shard_levels(rng, dims, cuts, low, largest):
    def one(axis_at, blocks):
        heights = jax.random.uniform(jax.random.fold_in(jax.random.fold_in(rng, 6), axis_at), (blocks,), jnp.float32, low / len(cuts), largest / len(cuts))
        return jnp.repeat(jnp.exp(heights), dims[axis_at] // blocks).reshape((-1,) + (1,) * (len(dims) - axis_at - 1))

    gain = one(*cuts[0])
    for cut in cuts[1:]:
        gain = gain * one(*cut)
    return gain


def bell_draw(key, shape, scale, bound, cuts=(), kind=jnp.bfloat16):
    values = jax.random.normal(key, shape, jnp.float32) * scale
    if len(cuts) > 0:
        values = shard_levels(key, shape, cuts, -0.22, 0.18) * values
    return jnp.clip(values, min=-bound, max=bound).astype(kind)


def bell_draw_with(stream_key, shape, scale, most, split, heavy, held_as=jnp.bfloat16):
    array = scale * jax.random.normal(stream_key, shape, jnp.float32)
    if split:
        array = array * shard_levels(stream_key, shape, split, -0.22, 0.18)
    return jnp.clip(with_spikes(array, jax.random.fold_in(stream_key, 3), *heavy), -most, most).astype(held_as)


def setup_inputs(seed: int = 0) -> dict:
    key_list = jax.random.split(jax.random.key(seed), 6)
    master_gate = bell_draw_with(key_list[0], (EXPERTS, D_MODEL, D_EXPERT), D_MODEL ** -0.5, 0.25, ((0, 4), (1, 32)), (1, 2, 32, 2.75), jnp.float32)
    master_up = bell_draw_with(key_list[1], (EXPERTS, D_MODEL, D_EXPERT), D_MODEL ** -0.5, 0.25, ((0, 4), (1, 32)), (1, 2, 32, 2.75), jnp.float32)
    master_down = bell_draw_with(key_list[2], (EXPERTS, D_EXPERT, D_MODEL), D_EXPERT ** -0.5, 0.3125, ((0, 4), (2, 32)), (2, 1, 32, 2.75), jnp.float32)
    router_weight = bell_draw(key_list[3], (D_MODEL, EXPERTS), D_MODEL ** -0.5, 0.125, ((0, 32), (1, 4)), jnp.float32)
    router_gain = jnp.clip(1.0 + 0.15 * jax.random.normal(key_list[4], (D_MODEL,), jnp.float32), 0.25, 1.75)
    return dict(master_gate=master_gate, master_up=master_up, master_down=master_down, router_weight=router_weight, router_gain=router_gain)


def reference(master_gate, master_up, master_down, router_weight, router_gain):
    scale_gate = jnp.max(jnp.abs(master_gate), axis=1)
    final_gate = (master_gate / jnp.expand_dims(scale_gate, 1)).astype(jnp.bfloat16)
    scale_up = jnp.max(jnp.abs(master_up), axis=1)
    final_up = (master_up / jnp.expand_dims(scale_up, 1)).astype(jnp.bfloat16)
    scale_down = jnp.max(jnp.abs(master_down), axis=2)
    final_down = (master_down / jnp.expand_dims(scale_down, 2)).astype(jnp.bfloat16)
    serve_router = (router_weight * router_gain[:, None]).astype(jnp.bfloat16)
    return final_gate, final_up, final_down, scale_gate, scale_up, scale_down, serve_router
```

```python
import jax
import jax.numpy as jnp
from jax import lax
from jax.experimental import pallas as pl
from jax.experimental.pallas import tpu as pltpu
from jax.sharding import PartitionSpec as P

MESH = pl.DeviceIdType.MESH
E, R, C, K = 16, 64, 1408, 44
S = 32
LT = C // 128
NT = 2 * LT
PIECE = K * 8
CHIPS = [(1, 0), (0, 1), (3, 0), (0, 3), (2, 2), (1, 1), (3, 3), (1, 3), (3, 1), (2, 1), (1, 2), (2, 3), (3, 2), (2, 0), (0, 2)]
OFFSETS = [(z, x, 0) for z, x in CHIPS] + [(z, x, 1) for z, x in CHIPS] + [(0, 0, 1)]


def target(me, offset):
    z, x, core = me // 8, (me // 2) % 4, me % 2
    return ((z + offset[0]) % 4) * 8 + ((x + offset[1]) % 4) * 2 + (core + offset[2]) % 2


def greet(ex, me, experts):
    barrier = pltpu.get_barrier_semaphore()
    for offset in OFFSETS:
        pl.semaphore_signal(barrier, inc=1, device_id=(ex, target(me, offset)), device_id_type=MESH)
    if experts:
        for i in range(1, 4):
            pl.semaphore_signal(barrier, inc=1, device_id=((ex + i) % 4, me), device_id_type=MESH)
    pl.semaphore_wait(barrier, S - 1 + (3 if experts else 0))


def await_bytes(ref, sem):
    pltpu.make_async_copy(ref, ref, sem).wait()


def maxima_kernel(gate, up, down, weight, gain, tops, part):
    for a, x in enumerate((gate, up, down)):
        for half in range(2):
            tops[half, 0, a] = jnp.max(jnp.abs(x[8 * half : 8 * half + 8]), axis=1)
    scaled = weight[...] * gain[...]
    part[...] = jnp.concatenate([scaled, jnp.zeros_like(scaled)], axis=1).astype(jnp.bfloat16)


def maxima(gate, up, down, weight, gain):
    rows = pl.BlockSpec((E, R, 128), lambda i: (0, 0, i))
    return pl.pallas_call(
        maxima_kernel,
        name="maxima",
        grid=(LT,),
        in_specs=[rows, rows, rows, pl.BlockSpec((E, R), lambda i: (0, 0)), pl.BlockSpec((1, R), lambda i: (0, 0))],
        out_specs=[pl.BlockSpec((2, 1, 3, 8, 128), lambda i: (0, i, 0, 0, 0)), pl.BlockSpec((E, 128), lambda i: (0, 0))],
        out_shape=[jax.ShapeDtypeStruct((2, LT, 3, 8, 128), jnp.float32), jax.ShapeDtypeStruct((E, 128), jnp.bfloat16)],
    )(gate, up, down, weight, gain)


def agree_kernel(tops, part, scale, router, landed, in_send, in_recv, out_send, out_recv, r_send, r_recv):
    me, ex = lax.axis_index("shard"), lax.axis_index("expert")
    greet(ex, me, False)

    def copy(src, dst, send, recv, to):
        return pltpu.make_async_remote_copy(
            src_ref=src, dst_ref=dst, send_sem=send, recv_sem=recv, device_id=(ex, to), device_id_type=MESH
        )

    def give(i, _):
        to = (me + i) % S

        @pl.when(to < NT)
        def _():
            copy(tops.at[to], landed.at[me], in_send, in_recv, to).start()

        return 0

    lax.fori_loop(1, S, give, 0)

    def share(i, _):
        copy(part, router.at[me], r_send, r_recv, (me + i) % S).start()
        return 0

    lax.fori_loop(1, S, share, 0)
    router[me] = part[...]

    @pl.when(me < NT)
    def _():
        landed[me] = tops[me]
        await_bytes(landed.at[pl.ds(0, S - 1)], in_recv)
        scale[me] = jnp.max(landed[...], axis=0)

        def tell(i, _):
            copy(scale.at[me], scale.at[me], out_send, out_recv, (me + i) % S).start()
            return 0

        lax.fori_loop(1, S, tell, 0)
        await_bytes(scale.at[pl.ds(0, NT - 1)], in_send)
        await_bytes(landed.at[pl.ds(0, S - 1)], out_send)
        await_bytes(scale.at[pl.ds(0, NT - 1)], out_recv)

    @pl.when(me >= NT)
    def _():
        await_bytes(scale, in_send)
        await_bytes(scale, out_recv)

    await_bytes(router.at[pl.ds(0, S - 1)], r_send)
    await_bytes(router.at[pl.ds(0, S - 1)], r_recv)


def agree(tops, part):
    vmem = pl.BlockSpec(memory_space=pltpu.VMEM)
    return pl.pallas_call(
        agree_kernel,
        name="agree",
        in_specs=[vmem, vmem],
        out_specs=[vmem, vmem],
        out_shape=[
            jax.ShapeDtypeStruct((NT, 3, 8, 128), jnp.float32),
            jax.ShapeDtypeStruct((S, E, 128), jnp.bfloat16),
        ],
        scratch_shapes=[pltpu.VMEM((S, 3, 8, 128), jnp.float32)] + [pltpu.SemaphoreType.DMA] * 6,
        compiler_params=pltpu.CompilerParams(collective_id=0, has_side_effects=True),
    )(tops.reshape(NT, 3, 8, 128), part)


def turn_kernel(gate, up, down, scale, out, turned):
    for a, x in enumerate((gate, up, down)):
        for p in range(8):
            low = x[p] * (1.0 / scale[0, 0, a, p : p + 1])
            high = x[p + 8] * (1.0 / scale[1, 0, a, p : p + 1])
            turned[a, pl.ds(p, 128, stride=8)] = jnp.concatenate([low, high], axis=0).T
        out[a] = turned[a].astype(jnp.bfloat16)


def turn(gate, up, down, scale):
    rows = pl.BlockSpec((E, R, 128), lambda i: (0, 0, i))
    return pl.pallas_call(
        turn_kernel,
        name="turn",
        grid=(LT,),
        in_specs=[rows, rows, rows, pl.BlockSpec((2, 1, 3, 8, 128), lambda i: (0, i, 0, 0, 0))],
        out_specs=pl.BlockSpec((3, 1024, 128), lambda i: (0, i, 0)),
        out_shape=jax.ShapeDtypeStruct((3, C * 8, 128), jnp.bfloat16),
        scratch_shapes=[pltpu.VMEM((3, 1024, 128), jnp.float32)],
    )(gate, up, down, scale.reshape(2, LT, 3, 8, 128))


def exchange_kernel(turned, router, pieces, routers, send, recv, r_send, r_recv, own):
    me, ex = lax.axis_index("shard"), lax.axis_index("expert")
    greet(ex, me, True)
    for i in range(1, 4):
        pltpu.make_async_remote_copy(
            src_ref=router, dst_ref=routers.at[ex], send_sem=r_send, recv_sem=r_recv,
            device_id=((ex + i) % 4, me), device_id_type=MESH,
        ).start()

    def send_all(a, _):
        for offset in OFFSETS:
            to = target(me, offset)
            pltpu.make_async_remote_copy(
                src_ref=turned.at[a, to], dst_ref=pieces.at[a, me], send_sem=send, recv_sem=recv,
                device_id=(ex, to), device_id_type=MESH,
            ).start()
        return 0

    lax.fori_loop(0, 3, send_all, 0)
    mine = [pltpu.make_async_copy(turned.at[a, me], pieces.at[a, me], own.at[a]) for a in range(3)]
    mine.append(pltpu.make_async_copy(router, routers.at[ex], own.at[3]))
    for copy in mine:
        copy.start()
    for copy in mine:
        copy.wait()
    await_bytes(routers.at[pl.ds(0, 3)], r_send)
    await_bytes(routers.at[pl.ds(0, 3)], r_recv)
    await_bytes(pieces.at[:, pl.ds(0, S - 1)], send)
    await_bytes(pieces.at[:, pl.ds(0, S - 1)], recv)


def exchange(turned, router):
    hbm = pl.BlockSpec(memory_space=pltpu.HBM)
    return pl.pallas_call(
        exchange_kernel,
        name="exchange",
        in_specs=[hbm, pl.BlockSpec(memory_space=pltpu.VMEM)],
        out_specs=[hbm, hbm],
        out_shape=[
            jax.ShapeDtypeStruct((3, S, PIECE, 128), jnp.bfloat16),
            jax.ShapeDtypeStruct((4, S, E, 128), jnp.bfloat16),
        ],
        scratch_shapes=[pltpu.SemaphoreType.DMA] * 4 + [pltpu.SemaphoreType.DMA((4,))],
        compiler_params=pltpu.CompilerParams(collective_id=1, has_side_effects=True),
    )(turned.reshape(3, S, PIECE, 128), router)


def halves(a, b):
    left = lax.broadcasted_iota(jnp.int32, a.shape, a.ndim - 1) < 64
    return jnp.where(left, a, pltpu.roll(b, 64, a.ndim - 1)), jnp.where(left, pltpu.roll(a, 64, a.ndim - 1), b)


def merge_kernel(width, pieces, routers, scale, gate, up, down, s_gate, s_up, s_down, serve):
    for a, out in enumerate((gate, up, down)):
        for j in range(width):
            pair = [pieces[a, 2 * j + i].astype(jnp.float32) for i in range(2)]
            low, high = halves(*pair)
            both = jnp.concatenate([low.reshape(K, 8, 128), high.reshape(K, 8, 128)], axis=1)
            out[:, :, 128 * j : 128 * j + 128] = both.astype(jnp.bfloat16)
    for j in range(width):
        pair = [routers[:, 2 * j + i].astype(jnp.float32).reshape(64, 128) for i in range(2)]
        serve[:, 128 * j : 128 * j + 128] = halves(*pair)[0].astype(jnp.bfloat16)

    @pl.when(pl.program_id(0) == 0)
    def _():
        start = lax.axis_index("shard") * K
        for a, out in enumerate((s_gate, s_up, s_down)):
            rows = [jnp.concatenate([scale[half, i, a] for i in range(LT)], axis=1) for half in range(2)]
            out[...] = pltpu.roll(jnp.concatenate(rows, axis=0), (C - start) % C, 1)[:, :K]


def merge(pieces, routers, scale):
    width = 2
    wide = pl.BlockSpec((K, E, 128 * width), lambda i: (0, 0, i))
    small = pl.BlockSpec((E, K), lambda i: (0, 0))
    return pl.pallas_call(
        lambda *refs: merge_kernel(width, *refs),
        name="merge",
        grid=(16 // width,),
        in_specs=[
            pl.BlockSpec((3, 2 * width, PIECE, 128), lambda i: (0, i, 0, 0)),
            pl.BlockSpec((4, 2 * width, E, 128), lambda i: (0, i, 0, 0)),
            pl.BlockSpec((2, LT, 3, 8, 128), lambda i: (0, 0, 0, 0, 0)),
        ],
        out_specs=[wide] * 3 + [small] * 3 + [pl.BlockSpec((64, 128 * width), lambda i: (0, i))],
        out_shape=[jax.ShapeDtypeStruct((K, E, 2048), jnp.bfloat16)] * 3
        + [jax.ShapeDtypeStruct((E, K), jnp.float32)] * 3
        + [jax.ShapeDtypeStruct((64, 2048), jnp.bfloat16)],
    )(pieces, routers, scale.reshape(2, LT, 3, 8, 128))


def body(master_gate, master_up, master_down, router_weight, router_gain):
    masters = (master_gate, master_up, jnp.swapaxes(master_down, 1, 2))
    tops, part = maxima(*masters, router_weight.T, router_gain[None])
    scale, router = agree(tops, part)
    pieces, routers = exchange(turn(*masters, scale), router)
    gate, up, down, s_gate, s_up, s_down, serve = merge(pieces, routers, scale)
    return (
        jnp.transpose(gate, (1, 2, 0)),
        jnp.transpose(up, (1, 2, 0)),
        jnp.transpose(down, (1, 0, 2)),
        s_gate,
        s_up,
        s_down,
        serve.T,
    )


def solution(mesh):
    return jax.shard_map(
        body,
        mesh=mesh,
        in_specs=(
            P("expert", "shard", None),
            P("expert", "shard", None),
            P("expert", None, "shard"),
            P("shard", "expert"),
            P("shard"),
        ),
        out_specs=(
            P("expert", None, "shard"),
            P("expert", None, "shard"),
            P("expert", "shard", None),
            P("expert", "shard"),
            P("expert", "shard"),
            P("expert", "shard"),
            P(),
        ),
        check_vma=False,
    )
```

```python
import jax
import jax.numpy as jnp
from jax import lax
from jax.experimental import pallas as pl
from jax.experimental.pallas import tpu as pltpu
from jax.sharding import PartitionSpec as P

MESH = pl.DeviceIdType.MESH
E, R, C, K = 16, 64, 1408, 44
S = 32
LT = C // 128
NT = 2 * LT
OUT = pltpu.VMEM
PIECE = K * 8
CHIPS = [(1, 0), (0, 1), (3, 0), (0, 3), (2, 2), (1, 1), (3, 3), (1, 3), (3, 1), (2, 1), (1, 2), (2, 3), (3, 2), (2, 0), (0, 2)]
OFFSETS = [(z, x, 0) for z, x in CHIPS] + [(z, x, 1) for z, x in CHIPS] + [(0, 0, 1)]


def target(me, offset):
    z, x, core = me // 8, (me // 2) % 4, me % 2
    return ((z + offset[0]) % 4) * 8 + ((x + offset[1]) % 4) * 2 + (core + offset[2]) % 2


def await_bytes(ref, sem):
    pltpu.make_async_copy(ref, ref, sem).wait()


def send_to(src, dst, send, recv, ex, to):
    pltpu.make_async_remote_copy(
        src_ref=src, dst_ref=dst, send_sem=send, recv_sem=recv, device_id=(ex, to), device_id_type=MESH
    ).start()


def relay_kernel(
    gate, up, down, weight, gain, pieces, routers, scale,
    x, turned, block, tops, landed, part, router,
    load, in_send, in_recv, out_send, out_recv, send, recv, r_send, r_recv, y_send, y_recv,
):
    me, ex = lax.axis_index("shard"), lax.axis_index("expert")
    loads = [pltpu.make_async_copy(src, x.at[a], load.at[a]) for a, src in enumerate((gate, up, down))]
    for copy in loads:
        copy.start()
    barrier = pltpu.get_barrier_semaphore()
    for offset in OFFSETS:
        pl.semaphore_signal(barrier, inc=1, device_id=(ex, target(me, offset)), device_id_type=MESH)
    for i in range(1, 4):
        pl.semaphore_signal(barrier, inc=1, device_id=((ex + i) % 4, me), device_id_type=MESH)
    scaled = weight[...] * gain[...]
    part[...] = jnp.concatenate([scaled, jnp.zeros_like(scaled)], axis=1).astype(jnp.bfloat16)
    router[me] = part[...]

    for a in range(3):
        loads[a].wait()

        def largest(i, _):
            lanes = pl.ds(pl.multiple_of(i * 128, 128), 128)
            for half in range(2):
                tops[a, half * LT + i] = jnp.max(jnp.abs(x[a, 8 * half : 8 * half + 8, :, lanes]), axis=1)
            return 0

        lax.fori_loop(0, LT, largest, 0)
        if a == 0:
            pl.semaphore_wait(barrier, S + 2)

        def give(i, _):
            to = (me + i) % S

            @pl.when(to < NT)
            def _():
                send_to(tops.at[a, to], landed.at[a, me], in_send, in_recv.at[a], ex, to)

            return 0

        lax.fori_loop(1, S, give, 0)

    def reduced(a, _):
        @pl.when(me < NT)
        def _():
            landed[a, me] = tops[a, me]
            await_bytes(landed.at[a, pl.ds(0, S - 1)], in_recv.at[a])
            scale[a, me] = jnp.max(landed[a], axis=0)

            def tell(i, _):
                send_to(scale.at[a, me], scale.at[a, me], out_send, out_recv.at[a], ex, (me + i) % S)
                return 0

            lax.fori_loop(1, S, tell, 0)

        return 0

    lax.fori_loop(0, 3, reduced, 0)

    def share(i, _):
        send_to(part, router.at[me], r_send, r_recv, ex, (me + i) % S)
        return 0

    lax.fori_loop(1, S, share, 0)

    def serve(a, _):
        @pl.when(me < NT)
        def _():
            await_bytes(scale.at[a, pl.ds(0, NT - 1)], out_recv.at[a])

        @pl.when(me >= NT)
        def _():
            await_bytes(scale.at[a], out_recv.at[a])

        def turn(i, _):
            lanes = pl.ds(pl.multiple_of(i * 128, 128), 128)
            by = [1.0 / scale[a, half * LT + i] for half in range(2)]
            for p in range(8):
                rows = [x[a, p + 8 * half, :, lanes] * by[half][p : p + 1] for half in range(2)]
                block[pl.ds(p, 128, stride=8)] = jnp.concatenate(rows, axis=0).T
            turned[a, pl.ds(pl.multiple_of(i * 1024, 1024), 1024)] = block[...].astype(jnp.bfloat16)
            return 0

        lax.fori_loop(0, LT, turn, 0)
        for offset in OFFSETS:
            to = target(me, offset)
            rows = pl.ds(pl.multiple_of(to * PIECE, PIECE), PIECE)
            send_to(turned.at[a, rows], pieces.at[a, me], send, recv, ex, to)
        pieces[a, me] = turned[a, pl.ds(pl.multiple_of(me * PIECE, PIECE), PIECE)]
        return 0

    lax.fori_loop(0, 3, serve, 0)
    await_bytes(router.at[pl.ds(0, S - 1)], r_recv)
    for i in range(1, 4):
        pltpu.make_async_remote_copy(
            src_ref=router, dst_ref=routers.at[ex], send_sem=y_send, recv_sem=y_recv,
            device_id=((ex + i) % 4, me), device_id_type=MESH,
        ).start()
    routers[ex] = router[...]

    @pl.when(me < NT)
    def _():
        await_bytes(tops.at[:, pl.ds(0, NT - 1)], in_send)
        await_bytes(landed.at[:, pl.ds(0, S - 1)], out_send)

    @pl.when(me >= NT)
    def _():
        await_bytes(tops, in_send)

    await_bytes(router.at[pl.ds(0, S - 1)], r_send)
    await_bytes(routers.at[pl.ds(0, 3)], y_send)
    await_bytes(routers.at[pl.ds(0, 3)], y_recv)
    await_bytes(pieces.at[:, pl.ds(0, S - 1)], send)
    await_bytes(pieces.at[:, pl.ds(0, S - 1)], recv)


def relay(gate, up, down, weight, gain):
    hbm, vmem = pl.BlockSpec(memory_space=pltpu.HBM), pl.BlockSpec(memory_space=pltpu.VMEM)
    dma = pltpu.SemaphoreType.DMA
    return pl.pallas_call(
        relay_kernel,
        name="relay",
        in_specs=[hbm, hbm, hbm, vmem, vmem],
        out_specs=[vmem, vmem, vmem],
        out_shape=[
            OUT((3, S, PIECE, 128), jnp.bfloat16),
            OUT((4, S, E, 128), jnp.bfloat16),
            OUT((3, NT, 8, 128), jnp.float32),
        ],
        scratch_shapes=[
            pltpu.VMEM((3, E, R, C), jnp.float32),
            pltpu.VMEM((3, C * 8, 128), jnp.bfloat16),
            pltpu.VMEM((1024, 128), jnp.float32),
            pltpu.VMEM((3, NT, 8, 128), jnp.float32),
            pltpu.VMEM((3, S, 8, 128), jnp.float32),
            pltpu.VMEM((E, 128), jnp.bfloat16),
            pltpu.VMEM((S, E, 128), jnp.bfloat16),
            dma((3,)), dma, dma((3,)), dma, dma((3,)), dma, dma, dma, dma, dma, dma,
        ],
        compiler_params=pltpu.CompilerParams(
            collective_id=0, has_side_effects=True, vmem_limit_bytes=40 * 2**20
        ),
    )(gate, up, down, weight, gain)


def halves(a, b):
    left = lax.broadcasted_iota(jnp.int32, a.shape, a.ndim - 1) < 64
    return jnp.where(left, a, pltpu.roll(b, 64, a.ndim - 1)), jnp.where(left, pltpu.roll(a, 64, a.ndim - 1), b)


def merge_kernel(width, pieces, routers, scale, gate, up, down, s_gate, s_up, s_down, serve):
    step = pl.program_id(0) * width
    for a, out in enumerate((gate, up, down)):
        for j in range(width):
            pair = [pieces[a, 2 * (step + j) + i].astype(jnp.float32) for i in range(2)]
            low, high = halves(*pair)
            both = jnp.concatenate([low.reshape(K, 8, 128), high.reshape(K, 8, 128)], axis=1)
            out[:, :, 128 * j : 128 * j + 128] = both.astype(jnp.bfloat16)
    for j in range(width):
        pair = [routers[:, 2 * (step + j) + i].astype(jnp.float32).reshape(64, 128) for i in range(2)]
        serve[:, 128 * j : 128 * j + 128] = halves(*pair)[0].astype(jnp.bfloat16)

    @pl.when(pl.program_id(0) == 0)
    def _():
        start = lax.axis_index("shard") * K
        for a, out in enumerate((s_gate, s_up, s_down)):
            rows = [jnp.concatenate([scale[a, half * LT + i] for i in range(LT)], axis=1) for half in range(2)]
            out[...] = pltpu.roll(jnp.concatenate(rows, axis=0), (C - start) % C, 1)[:, :K]


def merge(pieces, routers, scale):
    width = 2
    wide = pl.BlockSpec((K, E, 128 * width), lambda i: (0, 0, i))
    small = pl.BlockSpec((E, K), lambda i: (0, 0))
    vmem = pl.BlockSpec(memory_space=pltpu.VMEM)
    return pl.pallas_call(
        lambda *refs: merge_kernel(width, *refs),
        name="merge",
        grid=(16 // width,),
        in_specs=[vmem, vmem, vmem],
        out_specs=[wide] * 3 + [small] * 3 + [pl.BlockSpec((64, 128 * width), lambda i: (0, i))],
        out_shape=[jax.ShapeDtypeStruct((K, E, 2048), jnp.bfloat16)] * 3
        + [jax.ShapeDtypeStruct((E, K), jnp.float32)] * 3
        + [jax.ShapeDtypeStruct((64, 2048), jnp.bfloat16)],
        compiler_params=pltpu.CompilerParams(vmem_limit_bytes=16 * 2**20),
    )(pieces, routers, scale)


def body(master_gate, master_up, master_down, router_weight, router_gain):
    masters = (master_gate, master_up, jnp.swapaxes(master_down, 1, 2))
    pieces, routers, scale = relay(*masters, router_weight.T, router_gain[None])
    gate, up, down, s_gate, s_up, s_down, serve = merge(pieces, routers, scale)
    return (
        jnp.transpose(gate, (1, 2, 0)),
        jnp.transpose(up, (1, 2, 0)),
        jnp.transpose(down, (1, 0, 2)),
        s_gate,
        s_up,
        s_down,
        serve.T,
    )


def solution(mesh):
    return jax.shard_map(
        body,
        mesh=mesh,
        in_specs=(
            P("expert", "shard", None),
            P("expert", "shard", None),
            P("expert", None, "shard"),
            P("shard", "expert"),
            P("shard"),
        ),
        out_specs=(
            P("expert", None, "shard"),
            P("expert", None, "shard"),
            P("expert", "shard", None),
            P("expert", "shard"),
            P("expert", "shard"),
            P("expert", "shard"),
            P(),
        ),
        check_vma=False,
    )
```

```python
import jax
import jax.numpy as jnp
from jax import lax
from jax.experimental import pallas as pl
from jax.experimental.pallas import tpu as pltpu
from jax.sharding import PartitionSpec as P

MESH = pl.DeviceIdType.MESH
E, R, C, K = 16, 64, 1408, 44
S = 32
LT = C // 128
NT = 2 * LT
OUT = pltpu.VMEM
PIECE = K * 8
CHIPS = [(1, 1), (3, 3), (0, 1), (1, 3), (3, 1), (0, 3), (1, 0), (3, 0), (2, 0), (1, 2), (3, 2), (2, 2), (2, 1), (0, 2), (2, 3)]
OFFSETS = [(z, x, 0) for z, x in CHIPS] + [(z, x, 1) for z, x in CHIPS] + [(0, 0, 1)]


def target(me, offset):
    z, x, core = me // 8, (me // 2) % 4, me % 2
    return ((z + offset[0]) % 4) * 8 + ((x + offset[1]) % 4) * 2 + (core + offset[2]) % 2


def await_bytes(ref, sem):
    pltpu.make_async_copy(ref, ref, sem).wait()


def send_to(src, dst, send, recv, ex, to):
    pltpu.make_async_remote_copy(
        src_ref=src, dst_ref=dst, send_sem=send, recv_sem=recv, device_id=(ex, to), device_id_type=MESH
    ).start()


def halves(a, b):
    left = lax.broadcasted_iota(jnp.int32, a.shape, a.ndim - 1) < 64
    return jnp.where(left, a, pltpu.roll(b, 64, a.ndim - 1)), jnp.where(left, pltpu.roll(a, 64, a.ndim - 1), b)


def side_by_side(a, b):
    low, high = halves(a.astype(jnp.float32), b.astype(jnp.float32))
    both = jnp.concatenate([low.reshape(K, 8, 128), high.reshape(K, 8, 128)], axis=1)
    return both.astype(jnp.bfloat16)


def relay_kernel(
    gate, up, down, weight_in, gain_in, pieces, merged, routers, scale,
    x, weight, gain, turned, block, tops, landed, part, router,
    load, in_send, in_recv, out_send, out_recv, send, recv, r_send, r_recv, y_send, y_recv,
):
    me, ex = lax.axis_index("shard"), lax.axis_index("expert")
    firsts = [pltpu.make_async_copy(gate.at[pl.ds(8 * h, 8)], x.at[0, pl.ds(8 * h, 8)], load.at[h]) for h in range(2)]
    lates = [pltpu.make_async_copy(src, x.at[a], load.at[a + 1]) for a, src in ((1, up), (2, down))]
    smalls = [
        pltpu.make_async_copy(weight_in, weight, load.at[4]),
        pltpu.make_async_copy(gain_in, gain, load.at[5]),
    ]
    for copy in firsts + smalls:
        copy.start()
    barrier = pltpu.get_barrier_semaphore()
    for offset in OFFSETS:
        pl.semaphore_signal(barrier, inc=1, device_id=(ex, target(me, offset)), device_id_type=MESH)
    for i in range(1, 4):
        pl.semaphore_signal(barrier, inc=1, device_id=((ex + i) % 4, me), device_id_type=MESH)
    def largest(a, half):
        def one(i, _):
            lanes = pl.ds(pl.multiple_of(i * 128, 128), 128)
            tops[a, half * LT + i] = jnp.max(jnp.abs(x[a, 8 * half : 8 * half + 8, :, lanes]), axis=1)
            return 0

        lax.fori_loop(0, LT, one, 0)

    def give(a, half):
        def one(i, _):
            to = half * LT + (me + i) % LT

            @pl.when(to != me)
            def _():
                send_to(tops.at[a, to], landed.at[a, me], in_send, in_recv.at[a], ex, to)

            return 0

        lax.fori_loop(0, LT, one, 0)

    for half in range(2):
        firsts[half].wait()
        lates[half].start()
        largest(0, half)
        if half == 0:
            pl.semaphore_wait(barrier, S + 2)
        give(0, half)
    for a in (1, 2):
        lates[a - 1].wait()
        for half in range(2):
            largest(a, half)
            give(a, half)

    def reduced(a, _):
        @pl.when(me < NT)
        def _():
            landed[a, me] = tops[a, me]
            await_bytes(landed.at[a, pl.ds(0, S - 1)], in_recv.at[a])
            scale[a, me] = jnp.max(landed[a], axis=0)

            def tell(i, _):
                send_to(scale.at[a, me], scale.at[a, me], out_send, out_recv.at[a], ex, (me + i) % S)
                return 0

            lax.fori_loop(1, S, tell, 0)

        return 0

    lax.fori_loop(0, 3, reduced, 0)

    for copy in smalls:
        copy.wait()
    scaled = weight[...] * gain[...]
    part[...] = jnp.concatenate([scaled, jnp.zeros_like(scaled)], axis=1).astype(jnp.bfloat16)
    router[me] = part[...]

    def share(i, _):
        send_to(part, router.at[me], r_send, r_recv, ex, (me + i) % S)
        return 0

    lax.fori_loop(1, S, share, 0)

    def serve(a, _):
        @pl.when(me < NT)
        def _():
            await_bytes(scale.at[a, pl.ds(0, NT - 1)], out_recv.at[a])

        @pl.when(me >= NT)
        def _():
            await_bytes(scale.at[a], out_recv.at[a])

        def turn(i, _):
            lanes = pl.ds(pl.multiple_of(i * 128, 128), 128)
            by = [1.0 / scale[a, half * LT + i] for half in range(2)]
            for p in range(8):
                rows = [x[a, p + 8 * half, :, lanes] * by[half][p : p + 1] for half in range(2)]
                block[pl.ds(p, 128, stride=8)] = jnp.concatenate(rows, axis=0).T
            turned[a, pl.ds(pl.multiple_of(i * 1024, 1024), 1024)] = block[...].astype(jnp.bfloat16)
            return 0

        lax.fori_loop(0, LT, turn, 0)
        for offset in OFFSETS:
            to = target(me, offset)
            rows = pl.ds(pl.multiple_of(to * PIECE, PIECE), PIECE)
            send_to(turned.at[a, rows], pieces.at[a, me], send, recv.at[a], ex, to)
        pieces[a, me] = turned[a, pl.ds(pl.multiple_of(me * PIECE, PIECE), PIECE)]
        return 0

    lax.fori_loop(0, 3, serve, 0)
    await_bytes(router.at[pl.ds(0, S - 1)], r_recv)
    for i in range(1, 4):
        pltpu.make_async_remote_copy(
            src_ref=router, dst_ref=routers.at[ex], send_sem=y_send, recv_sem=y_recv,
            device_id=((ex + i) % 4, me), device_id_type=MESH,
        ).start()
    routers[ex] = router[...]

    def join(a, _):
        await_bytes(pieces.at[a, pl.ds(0, S - 1)], recv.at[a])

        def pair(j, _):
            lanes = pl.ds(pl.multiple_of(j * 128, 128), 128)
            merged[a, :, :, lanes] = side_by_side(pieces[a, 2 * j], pieces[a, 2 * j + 1])
            return 0

        lax.fori_loop(0, S // 2, pair, 0)
        return 0

    lax.fori_loop(0, 2, join, 0)

    @pl.when(me < NT)
    def _():
        await_bytes(tops.at[:, pl.ds(0, NT - 1)], in_send)
        await_bytes(landed.at[:, pl.ds(0, S - 1)], out_send)

    @pl.when(me >= NT)
    def _():
        await_bytes(tops, in_send)

    await_bytes(router.at[pl.ds(0, S - 1)], r_send)
    await_bytes(routers.at[pl.ds(0, 3)], y_send)
    await_bytes(routers.at[pl.ds(0, 3)], y_recv)
    await_bytes(pieces.at[:, pl.ds(0, S - 1)], send)
    await_bytes(pieces.at[2, pl.ds(0, S - 1)], recv.at[2])


def relay(gate, up, down, weight, gain):
    hbm, vmem = pl.BlockSpec(memory_space=pltpu.HBM), pl.BlockSpec(memory_space=pltpu.VMEM)
    dma = pltpu.SemaphoreType.DMA
    return pl.pallas_call(
        relay_kernel,
        name="relay",
        in_specs=[hbm] * 5,
        out_specs=[vmem] * 4,
        out_shape=[
            OUT((3, S, PIECE, 128), jnp.bfloat16),
            OUT((2, K, E, 2048), jnp.bfloat16),
            OUT((4, S, E, 128), jnp.bfloat16),
            OUT((3, NT, 8, 128), jnp.float32),
        ],
        scratch_shapes=[
            pltpu.VMEM((3, E, R, C), jnp.float32),
            pltpu.VMEM((E, R), jnp.float32),
            pltpu.VMEM((1, R), jnp.float32),
            pltpu.VMEM((3, C * 8, 128), jnp.bfloat16),
            pltpu.VMEM((1024, 128), jnp.float32),
            pltpu.VMEM((3, NT, 8, 128), jnp.float32),
            pltpu.VMEM((3, S, 8, 128), jnp.float32),
            pltpu.VMEM((E, 128), jnp.bfloat16),
            pltpu.VMEM((S, E, 128), jnp.bfloat16),
            dma((6,)), dma, dma((3,)), dma, dma((3,)), dma, dma((3,)), dma, dma, dma, dma,
        ],
        compiler_params=pltpu.CompilerParams(
            collective_id=0, has_side_effects=True, vmem_limit_bytes=40 * 2**20
        ),
    )(gate, up, down, weight, gain)


def finish_kernel(pieces, merged, routers, scale, gate, up, down, s_gate, s_up, s_down, serve, last, out_sem):
    outs = [pltpu.make_async_copy(merged.at[a], out, out_sem.at[a]) for a, out in enumerate((gate, up))]
    for copy in outs:
        copy.start()

    for part in range(4):

        def pair(j, _):
            lanes = pl.ds(pl.multiple_of(j * 128, 128), 128)
            last[:, :, lanes] = side_by_side(pieces[2, 2 * j], pieces[2, 2 * j + 1])
            return 0

        lax.fori_loop(4 * part, 4 * part + 4, pair, 0)
        lanes = pl.ds(512 * part, 512)
        outs.append(pltpu.make_async_copy(last.at[:, :, lanes], down.at[:, :, lanes], out_sem.at[2 + part]))
        outs[-1].start()
    for j in range(S // 2):
        both = [routers[:, 2 * j + i].astype(jnp.float32).reshape(64, 128) for i in range(2)]
        serve[:, 128 * j : 128 * j + 128] = halves(*both)[0].astype(jnp.bfloat16)
    start = lax.axis_index("shard") * K
    for a, out in enumerate((s_gate, s_up, s_down)):
        rows = [jnp.concatenate([scale[a, half * LT + i] for i in range(LT)], axis=1) for half in range(2)]
        out[...] = pltpu.roll(jnp.concatenate(rows, axis=0), (C - start) % C, 1)[:, :K]
    for copy in outs:
        copy.wait()


def finish(pieces, merged, routers, scale):
    hbm, vmem = pl.BlockSpec(memory_space=pltpu.HBM), pl.BlockSpec(memory_space=pltpu.VMEM)
    return pl.pallas_call(
        finish_kernel,
        name="finish",
        in_specs=[vmem] * 4,
        out_specs=[hbm] * 3 + [vmem] * 4,
        out_shape=[jax.ShapeDtypeStruct((K, E, 2048), jnp.bfloat16)] * 3
        + [jax.ShapeDtypeStruct((E, K), jnp.float32)] * 3
        + [jax.ShapeDtypeStruct((64, 2048), jnp.bfloat16)],
        scratch_shapes=[pltpu.VMEM((K, E, 2048), jnp.bfloat16), pltpu.SemaphoreType.DMA((6,))],
        compiler_params=pltpu.CompilerParams(vmem_limit_bytes=12 * 2**20),
    )(pieces, merged, routers, scale)


def body(master_gate, master_up, master_down, router_weight, router_gain):
    masters = (master_gate, master_up, jnp.swapaxes(master_down, 1, 2))
    pieces, merged, routers, scale = relay(*masters, router_weight.T, router_gain[None])
    gate, up, down, s_gate, s_up, s_down, serve = finish(pieces, merged, routers, scale)
    return (
        jnp.transpose(gate, (1, 2, 0)),
        jnp.transpose(up, (1, 2, 0)),
        jnp.transpose(down, (1, 0, 2)),
        s_gate,
        s_up,
        s_down,
        serve.T,
    )


def solution(mesh):
    return jax.shard_map(
        body,
        mesh=mesh,
        in_specs=(
            P("expert", "shard", None),
            P("expert", "shard", None),
            P("expert", None, "shard"),
            P("shard", "expert"),
            P("shard"),
        ),
        out_specs=(
            P("expert", None, "shard"),
            P("expert", None, "shard"),
            P("expert", "shard", None),
            P("expert", "shard"),
            P("expert", "shard"),
            P("expert", "shard"),
            P(),
        ),
        check_vma=False,
    )
```

```python
import jax
import jax.numpy as jnp
from jax import lax
from jax.experimental import pallas as pl
from jax.experimental.pallas import tpu as pltpu
from jax.sharding import PartitionSpec as P

MESH = pl.DeviceIdType.MESH
E, R, C, K = 16, 64, 1408, 44
S = 32
LT = C // 128
NT = 2 * LT
OUT = pltpu.VMEM
PIECE = K * 8
CHIPS = [(1, 1), (3, 3), (0, 1), (1, 3), (3, 1), (0, 3), (2, 0), (1, 0), (3, 0), (2, 2), (1, 2), (3, 2), (2, 1), (0, 2), (2, 3)]
OFFSETS = [(z, x, 0) for z, x in CHIPS] + [(z, x, 1) for z, x in CHIPS] + [(0, 0, 1)]


def target(me, offset):
    z, x, core = me // 8, (me // 2) % 4, me % 2
    return ((z + offset[0]) % 4) * 8 + ((x + offset[1]) % 4) * 2 + (core + offset[2]) % 2


def await_bytes(ref, sem):
    pltpu.make_async_copy(ref, ref, sem).wait()


def send_to(src, dst, send, recv, ex, to):
    pltpu.make_async_remote_copy(
        src_ref=src, dst_ref=dst, send_sem=send, recv_sem=recv, device_id=(ex, to), device_id_type=MESH
    ).start()


def halves(a, b):
    left = lax.broadcasted_iota(jnp.int32, a.shape, a.ndim - 1) < 64
    return jnp.where(left, a, pltpu.roll(b, 64, a.ndim - 1)), jnp.where(left, pltpu.roll(a, 64, a.ndim - 1), b)


def side_by_side(a, b):
    low, high = halves(a.astype(jnp.float32), b.astype(jnp.float32))
    both = jnp.concatenate([low.reshape(K, 8, 128), high.reshape(K, 8, 128)], axis=1)
    return both.astype(jnp.bfloat16)


def relay_kernel(
    gate, up, down, weight_in, gain_in, pieces, merged, routers, scale,
    x, weight, gain, turned, block, tops, landed, part, router,
    load, in_send, in_recv, out_send, out_recv, send, recv, r_send, r_recv, y_send, y_recv,
):
    me, ex = lax.axis_index("shard"), lax.axis_index("expert")
    firsts = [pltpu.make_async_copy(gate.at[pl.ds(8 * h, 8)], x.at[0, pl.ds(8 * h, 8)], load.at[h]) for h in range(2)]
    lates = [pltpu.make_async_copy(src, x.at[a], load.at[a + 1]) for a, src in ((1, up), (2, down))]
    smalls = [
        pltpu.make_async_copy(weight_in, weight, load.at[4]),
        pltpu.make_async_copy(gain_in, gain, load.at[5]),
    ]
    for copy in firsts + smalls:
        copy.start()
    barrier = pltpu.get_barrier_semaphore()
    for offset in OFFSETS:
        pl.semaphore_signal(barrier, inc=1, device_id=(ex, target(me, offset)), device_id_type=MESH)
    for i in range(1, 4):
        pl.semaphore_signal(barrier, inc=1, device_id=((ex + i) % 4, me), device_id_type=MESH)
    def largest(a, half):
        def one(i, _):
            lanes = pl.ds(pl.multiple_of(i * 128, 128), 128)
            tops[a, half * LT + i] = jnp.max(jnp.abs(x[a, 8 * half : 8 * half + 8, :, lanes]), axis=1)
            return 0

        lax.fori_loop(0, LT, one, 0)

    def give(a, half):
        def one(i, _):
            to = half * LT + (me + i) % LT

            @pl.when(to != me)
            def _():
                send_to(tops.at[a, to], landed.at[a, me], in_send, in_recv.at[a], ex, to)

            return 0

        lax.fori_loop(0, LT, one, 0)

    for half in range(2):
        firsts[half].wait()
        lates[half].start()
        largest(0, half)
        if half == 0:
            pl.semaphore_wait(barrier, S + 2)
        give(0, half)
    for a in (1, 2):
        lates[a - 1].wait()
        for half in range(2):
            largest(a, half)
            give(a, half)

    def reduced(a, _):
        @pl.when(me < NT)
        def _():
            landed[a, me] = tops[a, me]
            await_bytes(landed.at[a, pl.ds(0, S - 1)], in_recv.at[a])
            scale[a, me] = jnp.max(landed[a], axis=0)

            def tell(i, _):
                send_to(scale.at[a, me], scale.at[a, me], out_send, out_recv.at[a], ex, (me + i) % S)
                return 0

            lax.fori_loop(1, S, tell, 0)

        return 0

    lax.fori_loop(0, 3, reduced, 0)

    for copy in smalls:
        copy.wait()
    scaled = weight[...] * gain[...]
    part[...] = jnp.concatenate([scaled, jnp.zeros_like(scaled)], axis=1).astype(jnp.bfloat16)
    router[me] = part[...]

    def share(i, _):
        send_to(part, router.at[me], r_send, r_recv, ex, (me + i) % S)
        return 0

    lax.fori_loop(1, S, share, 0)

    def serve(a, _):
        @pl.when(me < NT)
        def _():
            await_bytes(scale.at[a, pl.ds(0, NT - 1)], out_recv.at[a])

        @pl.when(me >= NT)
        def _():
            await_bytes(scale.at[a], out_recv.at[a])

        def turn(i, block):
            lanes = pl.ds(i * 128, 128)
            by = [1.0 / scale[a, half * LT + i] for half in range(2)]
            for p in range(8):
                rows = [x[a, p + 8 * half, :, lanes] * by[half][p : p + 1] for half in range(2)]
                block[pl.ds(p, 128, stride=8)] = jnp.concatenate(rows, axis=0).T
            turned[a, pl.ds(i * 1024, 1024)] = block[...].astype(jnp.bfloat16)

        for i in range(LT):
            turn(i, block.at[i % 2])
        for offset in OFFSETS:
            to = target(me, offset)
            rows = pl.ds(pl.multiple_of(to * PIECE, PIECE), PIECE)
            send_to(turned.at[a, rows], pieces.at[a, me], send, recv.at[a], ex, to)
        pieces[a, me] = turned[a, pl.ds(pl.multiple_of(me * PIECE, PIECE), PIECE)]
        return 0

    lax.fori_loop(0, 3, serve, 0)
    await_bytes(router.at[pl.ds(0, S - 1)], r_recv)
    for i in range(1, 4):
        pltpu.make_async_remote_copy(
            src_ref=router, dst_ref=routers.at[ex], send_sem=y_send, recv_sem=y_recv,
            device_id=((ex + i) % 4, me), device_id_type=MESH,
        ).start()
    routers[ex] = router[...]

    def join(a, _):
        await_bytes(pieces.at[a, pl.ds(0, S - 1)], recv.at[a])

        def pair(j, _):
            lanes = pl.ds(pl.multiple_of(j * 128, 128), 128)
            merged[a, :, :, lanes] = side_by_side(pieces[a, 2 * j], pieces[a, 2 * j + 1])
            return 0

        lax.fori_loop(0, S // 2, pair, 0)
        return 0

    lax.fori_loop(0, 2, join, 0)

    @pl.when(me < NT)
    def _():
        await_bytes(tops.at[:, pl.ds(0, NT - 1)], in_send)
        await_bytes(landed.at[:, pl.ds(0, S - 1)], out_send)

    @pl.when(me >= NT)
    def _():
        await_bytes(tops, in_send)

    await_bytes(router.at[pl.ds(0, S - 1)], r_send)
    await_bytes(routers.at[pl.ds(0, 3)], y_send)
    await_bytes(routers.at[pl.ds(0, 3)], y_recv)
    await_bytes(pieces.at[:, pl.ds(0, S - 1)], send)
    await_bytes(pieces.at[2, pl.ds(0, S - 1)], recv.at[2])


def relay(gate, up, down, weight, gain):
    hbm, vmem = pl.BlockSpec(memory_space=pltpu.HBM), pl.BlockSpec(memory_space=pltpu.VMEM)
    dma = pltpu.SemaphoreType.DMA
    return pl.pallas_call(
        relay_kernel,
        name="relay",
        in_specs=[hbm] * 5,
        out_specs=[vmem] * 4,
        out_shape=[
            OUT((3, S, PIECE, 128), jnp.bfloat16),
            OUT((2, K, E, 2048), jnp.bfloat16),
            OUT((4, S, E, 128), jnp.bfloat16),
            OUT((3, NT, 8, 128), jnp.float32),
        ],
        scratch_shapes=[
            pltpu.VMEM((3, E, R, C), jnp.float32),
            pltpu.VMEM((E, R), jnp.float32),
            pltpu.VMEM((1, R), jnp.float32),
            pltpu.VMEM((3, C * 8, 128), jnp.bfloat16),
            pltpu.VMEM((2, 1024, 128), jnp.float32),
            pltpu.VMEM((3, NT, 8, 128), jnp.float32),
            pltpu.VMEM((3, S, 8, 128), jnp.float32),
            pltpu.VMEM((E, 128), jnp.bfloat16),
            pltpu.VMEM((S, E, 128), jnp.bfloat16),
            dma((6,)), dma, dma((3,)), dma, dma((3,)), dma, dma((3,)), dma, dma, dma, dma,
        ],
        compiler_params=pltpu.CompilerParams(
            collective_id=0, has_side_effects=True, vmem_limit_bytes=40 * 2**20
        ),
    )(gate, up, down, weight, gain)


def finish_kernel(pieces, merged, routers, scale, gate, up, down, s_gate, s_up, s_down, serve, last, out_sem):
    outs = [pltpu.make_async_copy(merged.at[a], out, out_sem.at[a]) for a, out in enumerate((gate, up))]
    for copy in outs:
        copy.start()

    for part in range(4):

        def pair(j, _):
            lanes = pl.ds(pl.multiple_of(j * 128, 128), 128)
            last[:, :, lanes] = side_by_side(pieces[2, 2 * j], pieces[2, 2 * j + 1])
            return 0

        lax.fori_loop(4 * part, 4 * part + 4, pair, 0)
        lanes = pl.ds(512 * part, 512)
        outs.append(pltpu.make_async_copy(last.at[:, :, lanes], down.at[:, :, lanes], out_sem.at[2 + part]))
        outs[-1].start()
    for j in range(S // 2):
        both = [routers[:, 2 * j + i].astype(jnp.float32).reshape(64, 128) for i in range(2)]
        serve[:, 128 * j : 128 * j + 128] = halves(*both)[0].astype(jnp.bfloat16)
    start = lax.axis_index("shard") * K
    for a, out in enumerate((s_gate, s_up, s_down)):
        rows = [jnp.concatenate([scale[a, half * LT + i] for i in range(LT)], axis=1) for half in range(2)]
        out[...] = pltpu.roll(jnp.concatenate(rows, axis=0), (C - start) % C, 1)[:, :K]
    for copy in outs:
        copy.wait()


def finish(pieces, merged, routers, scale):
    hbm, vmem = pl.BlockSpec(memory_space=pltpu.HBM), pl.BlockSpec(memory_space=pltpu.VMEM)
    return pl.pallas_call(
        finish_kernel,
        name="finish",
        in_specs=[vmem] * 4,
        out_specs=[hbm] * 3 + [vmem] * 4,
        out_shape=[jax.ShapeDtypeStruct((K, E, 2048), jnp.bfloat16)] * 3
        + [jax.ShapeDtypeStruct((E, K), jnp.float32)] * 3
        + [jax.ShapeDtypeStruct((64, 2048), jnp.bfloat16)],
        scratch_shapes=[pltpu.VMEM((K, E, 2048), jnp.bfloat16), pltpu.SemaphoreType.DMA((6,))],
        compiler_params=pltpu.CompilerParams(vmem_limit_bytes=12 * 2**20),
    )(pieces, merged, routers, scale)


def body(master_gate, master_up, master_down, router_weight, router_gain):
    masters = (master_gate, master_up, jnp.swapaxes(master_down, 1, 2))
    pieces, merged, routers, scale = relay(*masters, router_weight.T, router_gain[None])
    gate, up, down, s_gate, s_up, s_down, serve = finish(pieces, merged, routers, scale)
    return (
        jnp.transpose(gate, (1, 2, 0)),
        jnp.transpose(up, (1, 2, 0)),
        jnp.transpose(down, (1, 0, 2)),
        s_gate,
        s_up,
        s_down,
        serve.T,
    )


def solution(mesh):
    return jax.shard_map(
        body,
        mesh=mesh,
        in_specs=(
            P("expert", "shard", None),
            P("expert", "shard", None),
            P("expert", None, "shard"),
            P("shard", "expert"),
            P("shard"),
        ),
        out_specs=(
            P("expert", None, "shard"),
            P("expert", None, "shard"),
            P("expert", "shard", None),
            P("expert", "shard"),
            P("expert", "shard"),
            P("expert", "shard"),
            P(),
        ),
        check_vma=False,
    )
```

```python
import jax
import jax.numpy as jnp
from jax import lax
from jax.experimental import pallas as pl
from jax.experimental.pallas import tpu as pltpu
from jax.sharding import PartitionSpec as P

MESH = pl.DeviceIdType.MESH
E, R, C, K = 16, 64, 1408, 44
S = 32
LT = C // 128
NT = 2 * LT
OUT = pltpu.VMEM
PIECE = K * 8
CHIPS = [(1, 1), (3, 3), (0, 1), (1, 3), (3, 1), (0, 3), (2, 0), (1, 0), (3, 0), (2, 2), (1, 2), (3, 2), (2, 1), (0, 2), (2, 3)]
OFFSETS = [(z, x, 0) for z, x in CHIPS] + [(z, x, 1) for z, x in CHIPS] + [(0, 0, 1)]


def target(me, offset):
    z, x, core = me // 8, (me // 2) % 4, me % 2
    return ((z + offset[0]) % 4) * 8 + ((x + offset[1]) % 4) * 2 + (core + offset[2]) % 2


def await_bytes(ref, sem):
    pltpu.make_async_copy(ref, ref, sem).wait()


def send_to(src, dst, send, recv, ex, to):
    pltpu.make_async_remote_copy(
        src_ref=src, dst_ref=dst, send_sem=send, recv_sem=recv, device_id=(ex, to), device_id_type=MESH
    ).start()


def halves(a, b):
    left = lax.broadcasted_iota(jnp.int32, a.shape, a.ndim - 1) < 64
    return jnp.where(left, a, pltpu.roll(b, 64, a.ndim - 1)), jnp.where(left, pltpu.roll(a, 64, a.ndim - 1), b)


def side_by_side(a, b):
    low, high = halves(a.astype(jnp.float32), b.astype(jnp.float32))
    both = jnp.concatenate([v.reshape(-1, 8, 128) for v in (low, high)], axis=1)
    return both.astype(jnp.bfloat16)


def relay_kernel(
    gate, up, down, weight_in, gain_in, pieces, merged, whole, mine,
    routers, scale, x, weight, gain, turned, block, tops, landed, part, router,
    load, in_send, in_recv, out_send, out_recv, send, recv, r_send, r_recv, y_send, y_recv,
):
    me, ex = lax.axis_index("shard"), lax.axis_index("expert")
    firsts = [pltpu.make_async_copy(gate.at[pl.ds(8 * h, 8)], x.at[0, pl.ds(8 * h, 8)], load.at[h]) for h in range(2)]
    lates = [pltpu.make_async_copy(src, x.at[a], load.at[a + 1]) for a, src in ((1, up), (2, down))]
    smalls = [
        pltpu.make_async_copy(weight_in, weight, load.at[4]),
        pltpu.make_async_copy(gain_in, gain, load.at[5]),
    ]
    for copy in firsts + smalls:
        copy.start()
    barrier = pltpu.get_barrier_semaphore()
    for offset in OFFSETS:
        pl.semaphore_signal(barrier, inc=1, device_id=(ex, target(me, offset)), device_id_type=MESH)
    for i in range(1, 4):
        pl.semaphore_signal(barrier, inc=1, device_id=((ex + i) % 4, me), device_id_type=MESH)
    def largest(a, half):
        def one(i, _):
            lanes = pl.ds(pl.multiple_of(i * 128, 128), 128)
            tops[a, half * LT + i] = jnp.max(jnp.abs(x[a, 8 * half : 8 * half + 8, :, lanes]), axis=1)
            return 0

        lax.fori_loop(0, LT, one, 0)

    def give(a, half):
        def one(i, _):
            to = half * LT + (me + i) % LT

            @pl.when(to != me)
            def _():
                send_to(tops.at[a, to], landed.at[a, me], in_send, in_recv.at[a], ex, to)

            return 0

        lax.fori_loop(0, LT, one, 0)

    for half in range(2):
        firsts[half].wait()
        lates[half].start()
        largest(0, half)
        if half == 0:
            pl.semaphore_wait(barrier, S + 2)
        give(0, half)
    for a in (1, 2):
        lates[a - 1].wait()
        for half in range(2):
            largest(a, half)
            give(a, half)

    def reduced(a, _):
        @pl.when(me < NT)
        def _():
            landed[a, me] = tops[a, me]
            await_bytes(landed.at[a, pl.ds(0, S - 1)], in_recv.at[a])
            scale[a, me] = jnp.max(landed[a], axis=0)

            def tell(i, _):
                send_to(scale.at[a, me], scale.at[a, me], out_send, out_recv.at[a], ex, (me + i) % S)
                return 0

            lax.fori_loop(1, S, tell, 0)

        return 0

    lax.fori_loop(0, 3, reduced, 0)

    for copy in smalls:
        copy.wait()
    scaled = weight[...] * gain[...]
    part[...] = jnp.concatenate([scaled, jnp.zeros_like(scaled)], axis=1).astype(jnp.bfloat16)
    router[me] = part[...]

    def share(i, _):
        send_to(part, router.at[me], r_send, r_recv, ex, (me + i) % S)
        return 0

    lax.fori_loop(1, S, share, 0)

    def serve(a, _):
        @pl.when(me < NT)
        def _():
            await_bytes(scale.at[a, pl.ds(0, NT - 1)], out_recv.at[a])

        @pl.when(me >= NT)
        def _():
            await_bytes(scale.at[a], out_recv.at[a])

        def turn(i, block):
            lanes = pl.ds(i * 128, 128)
            by = [1.0 / scale[a, half * LT + i] for half in range(2)]
            for p in range(8):
                rows = [x[a, p + 8 * half, :, lanes] * by[half][p : p + 1] for half in range(2)]
                block[pl.ds(p, 128, stride=8)] = jnp.concatenate(rows, axis=0).T
            turned[a, pl.ds(i * 1024, 1024)] = block[...].astype(jnp.bfloat16)

        for i in range(LT):
            turn(i, block.at[i % 2])
        for offset in OFFSETS:
            to = target(me, offset)
            rows = pl.ds(pl.multiple_of(to * PIECE, PIECE), PIECE)
            send_to(turned.at[a, rows], pieces.at[a, me], send, recv.at[a], ex, to)
        pieces[a, me] = turned[a, pl.ds(pl.multiple_of(me * PIECE, PIECE), PIECE)]
        return 0

    lax.fori_loop(0, 3, serve, 0)
    await_bytes(router.at[pl.ds(0, S - 1)], r_recv)
    for i in range(1, 4):
        pltpu.make_async_remote_copy(
            src_ref=router, dst_ref=routers.at[ex], send_sem=y_send, recv_sem=y_recv,
            device_id=((ex + i) % 4, me), device_id_type=MESH,
        ).start()
    routers[ex] = router[...]

    def join(a, _):
        await_bytes(pieces.at[a, pl.ds(0, S - 1)], recv.at[a])

        def pair(j, _):
            lanes = pl.ds(pl.multiple_of(j * 128, 128), 128)
            merged[a, :, :, lanes] = side_by_side(pieces[a, 2 * j], pieces[a, 2 * j + 1])
            return 0

        lax.fori_loop(0, S // 2, pair, 0)
        return 0

    lax.fori_loop(0, 2, join, 0)
    await_bytes(routers.at[pl.ds(0, 3)], y_recv)
    for j in range(S // 2):
        both = [routers[:, 2 * j + i].astype(jnp.float32).reshape(64, 128) for i in range(2)]
        whole[:, 128 * j : 128 * j + 128] = halves(*both)[0].astype(jnp.bfloat16)
    start = me * K
    for a in range(3):
        rows = [jnp.concatenate([scale[a, half * LT + i] for i in range(LT)], axis=1) for half in range(2)]
        mine[a] = pltpu.roll(jnp.concatenate(rows, axis=0), (C - start) % C, 1)[:, :128]

    @pl.when(me < NT)
    def _():
        await_bytes(tops.at[:, pl.ds(0, NT - 1)], in_send)
        await_bytes(landed.at[:, pl.ds(0, S - 1)], out_send)

    @pl.when(me >= NT)
    def _():
        await_bytes(tops, in_send)

    await_bytes(router.at[pl.ds(0, S - 1)], r_send)
    await_bytes(routers.at[pl.ds(0, 3)], y_send)
    await_bytes(pieces.at[:, pl.ds(0, S - 1)], send)
    await_bytes(pieces.at[2, pl.ds(0, S - 1)], recv.at[2])


def relay(gate, up, down, weight, gain):
    hbm, vmem = pl.BlockSpec(memory_space=pltpu.HBM), pl.BlockSpec(memory_space=pltpu.VMEM)
    dma = pltpu.SemaphoreType.DMA
    return pl.pallas_call(
        relay_kernel,
        name="relay",
        in_specs=[hbm] * 5,
        out_specs=[vmem] * 4,
        out_shape=[
            OUT((3, S, PIECE, 128), jnp.bfloat16),
            OUT((2, K, E, 2048), jnp.bfloat16),
            OUT((64, 2048), jnp.bfloat16),
            OUT((3, E, 128), jnp.float32),
        ],
        scratch_shapes=[
            pltpu.VMEM((4, S, E, 128), jnp.bfloat16),
            pltpu.VMEM((3, NT, 8, 128), jnp.float32),
            pltpu.VMEM((3, E, R, C), jnp.float32),
            pltpu.VMEM((E, R), jnp.float32),
            pltpu.VMEM((1, R), jnp.float32),
            pltpu.VMEM((3, C * 8, 128), jnp.bfloat16),
            pltpu.VMEM((2, 1024, 128), jnp.float32),
            pltpu.VMEM((3, NT, 8, 128), jnp.float32),
            pltpu.VMEM((3, S, 8, 128), jnp.float32),
            pltpu.VMEM((E, 128), jnp.bfloat16),
            pltpu.VMEM((S, E, 128), jnp.bfloat16),
            dma((6,)), dma, dma((3,)), dma, dma((3,)), dma, dma((3,)), dma, dma, dma, dma,
        ],
        compiler_params=pltpu.CompilerParams(
            collective_id=0, has_side_effects=True, vmem_limit_bytes=40 * 2**20
        ),
    )(gate, up, down, weight, gain)


def finish_kernel(pieces, merged, router, mine, gate, up, down, s_gate, s_up, s_down, serve, last, out_sem):
    outs = [pltpu.make_async_copy(merged.at[a], out, out_sem.at[a]) for a, out in enumerate((gate, up))]
    outs.append(pltpu.make_async_copy(router, serve, out_sem.at[4]))
    for copy in outs:
        copy.start()

    for part in range(2):
        rows, columns = slice(part * PIECE // 2, (part + 1) * PIECE // 2), pl.ds(part * K // 2, K // 2)

        def pair(j, _):
            lanes = pl.ds(pl.multiple_of(j * 128, 128), 128)
            last[columns, :, lanes] = side_by_side(pieces[2, 2 * j, rows], pieces[2, 2 * j + 1, rows])
            return 0

        lax.fori_loop(0, S // 2, pair, 0)
        outs.append(pltpu.make_async_copy(last.at[columns], down.at[columns], out_sem.at[2 + part]))
        outs[-1].start()
    for a, out in enumerate((s_gate, s_up, s_down)):
        out[...] = mine[a, :, :K]
    for copy in outs:
        copy.wait()


def finish(pieces, merged, router, mine):
    hbm, vmem = pl.BlockSpec(memory_space=pltpu.HBM), pl.BlockSpec(memory_space=pltpu.VMEM)
    return pl.pallas_call(
        finish_kernel,
        name="finish",
        in_specs=[vmem] * 4,
        out_specs=[hbm] * 3 + [vmem] * 3 + [hbm],
        out_shape=[jax.ShapeDtypeStruct((K, E, 2048), jnp.bfloat16)] * 3
        + [jax.ShapeDtypeStruct((E, K), jnp.float32)] * 3
        + [jax.ShapeDtypeStruct((64, 2048), jnp.bfloat16)],
        scratch_shapes=[pltpu.VMEM((K, E, 2048), jnp.bfloat16), pltpu.SemaphoreType.DMA((5,))],
        compiler_params=pltpu.CompilerParams(vmem_limit_bytes=12 * 2**20),
    )(pieces, merged, router, mine)


def body(master_gate, master_up, master_down, router_weight, router_gain):
    masters = (master_gate, master_up, jnp.swapaxes(master_down, 1, 2))
    pieces, merged, router, mine = relay(*masters, router_weight.T, router_gain[None])
    gate, up, down, s_gate, s_up, s_down, serve = finish(pieces, merged, router, mine)
    return (
        jnp.transpose(gate, (1, 2, 0)),
        jnp.transpose(up, (1, 2, 0)),
        jnp.transpose(down, (1, 0, 2)),
        s_gate,
        s_up,
        s_down,
        serve.T,
    )


def solution(mesh):
    return jax.shard_map(
        body,
        mesh=mesh,
        in_specs=(
            P("expert", "shard", None),
            P("expert", "shard", None),
            P("expert", None, "shard"),
            P("shard", "expert"),
            P("shard"),
        ),
        out_specs=(
            P("expert", None, "shard"),
            P("expert", None, "shard"),
            P("expert", "shard", None),
            P("expert", "shard"),
            P("expert", "shard"),
            P("expert", "shard"),
            P(),
        ),
        check_vma=False,
    )
```
